32 devices in a mesh: ctx: 8 (over y, x, core), tp: 4 (over z).
Axes of the slice: x: 2, y: 2, z: 4, core: 2. Of those that a mesh axis runs over, the one named last changes fastest.
Arguments:
- hidden_in: bfloat16 [2048, 4096], P(('ctx', 'tp')), may hold values from -6 to 6
- norm_gain: float32 [4096], replicated, may hold values from 0.5 to 1.5
- proj_weight: bfloat16 [4096, 4096], P(None, 'tp'), may hold values from -0.09375 to 0.09375
- conv_in: bfloat16 [2048, 4096], P('ctx', 'tp'), may hold values from -6 to 6
- conv_weight: float32 [4, 4096], P(None, 'tp'), may hold values from -3 to 3
- conv_bias: float32 [4096], P('tp'), may hold values from -3 to 3
- act_grad: bfloat16 [2048, 4096], P('ctx', 'tp'), may hold values from -6 to 6
Outputs:
- hidden_input_gradient: bfloat16 [2048, 4096], P(('ctx', 'tp'))
- norm_gain_gradient: float32 [4096], replicated
- taps_grad: float32 [4, 4096], P(None, 'tp')
- bias_grad: float32 [4096], P('tp')
The draws below stay inside these ranges and needn't reach their ends.
All inputs are finite; a program needn't handle non-finite values.
Results may differ from the reference program's by a relative error of at most 0.013.
Values may be sent and summed in bfloat16 or wider, within the bound.
No kernel may reach another device: no remote copies, remote signals or barrier semaphores. Data moves between devices by JAX's collectives and lax.ppermute only.
A program may use at most 64 MiB of HBM per device.

```python
import jax
import jax.numpy as jnp
from jax import lax

D = 4096
INNER_DEV = 1024
TAPS = 4
TOKENS = 2048
INNER = 4096
N_TP = 4


def block_levels(key, extent, pieces, low, largest):
    def one(dim, blocks):
        steps = jax.random.uniform(jax.random.fold_in(jax.random.fold_in(key, 6), dim), (blocks,), jnp.float32, low / len(pieces), largest / len(pieces))
        return jnp.repeat(jnp.exp(steps), extent[dim] // blocks).reshape((-1,) + (1,) * (len(extent) - dim - 1))

    loudness = one(*pieces[0])
    for cut in pieces[1:]:
        loudness = loudness * one(*cut)
    return loudness


def gaussian(key, dims, scale, reach, split=(), kind=jnp.bfloat16):
    factor_of = block_levels(key, dims, split, -0.22, 0.18) if split else 1.0
    values = jax.random.normal(key, dims, jnp.float32) * scale * factor_of
    return jnp.minimum(jnp.maximum(values, -reach), reach).astype(kind)


def setup_inputs(seed: int = 0) -> dict:
    seeds = jax.random.split(jax.random.key(seed), 8)
    hidden_in = gaussian(seeds[0], (TOKENS, D), 1.0, 6.0, ((0, 32),))
    norm_gain = jnp.clip(1.0 + 0.1 * jax.random.normal(seeds[1], (D,), jnp.float32), 0.5, 1.5)
    proj_weight = gaussian(seeds[2], (D, INNER), INNER ** -0.5, 0.09375, ((1, 4),))
    conv_in = gaussian(seeds[3], (TOKENS, INNER), 1.0, 6.0, ((0, 8), (1, 4)))
    conv_weight = gaussian(seeds[4], (TAPS, INNER), 0.5, 3.0, ((1, 4),), jnp.float32)
    conv_bias = gaussian(seeds[5], (INNER,), 0.5, 3.0, ((0, 4),), jnp.float32)
    act_grad = gaussian(seeds[6], (TOKENS, INNER), 1.0, 6.0, ((0, 8), (1, 4)))
    return {"hidden_in": hidden_in, "norm_gain": norm_gain, "proj_weight": proj_weight, "conv_in": conv_in, "conv_weight": conv_weight, "conv_bias": conv_bias, "act_grad": act_grad}


def channel_block(carry, items):
    saved, cotangent, taps, offset, weight = items
    count_tok = saved.shape[0]
    tap_count = taps.shape[0]
    padded = jnp.concatenate([jnp.zeros((tap_count - 1, saved.shape[1]), jnp.float32), saved.astype(jnp.float32)], 0)
    preact = offset[None, :] + sum((taps[index][None, :] * padded[tap_count - 1 - index:tap_count - 1 - index + count_tok] for index in range(tap_count)))
    sigmoid_v = jax.nn.sigmoid(preact)
    pre_grad = cotangent.astype(jnp.float32) * sigmoid_v * (1.0 + preact * (1.0 - sigmoid_v))
    taps_part = jnp.stack([lax.optimization_barrier(jnp.sum(pre_grad * padded[tap_count - 1 - index:tap_count - 1 - index + count_tok], 0)) for index in range(tap_count)], 0)
    bias_part = lax.optimization_barrier(jnp.sum(pre_grad, 0))
    after = jnp.concatenate([pre_grad, jnp.zeros((tap_count - 1, saved.shape[1]), jnp.float32)], 0)
    in_grad = sum((taps[index][None, :] * after[index:index + count_tok] for index in range(tap_count))).astype(jnp.bfloat16)
    part_grad = lax.dot_general(in_grad, weight, (((1,), (1,)), ((), ())), preferred_element_type=jnp.float32).astype(jnp.bfloat16)
    part_grad = lax.optimization_barrier(part_grad)
    carry = carry + part_grad.astype(jnp.float32)
    return (carry, (taps_part, bias_part))

def reference(hidden_in, norm_gain, proj_weight, conv_in, conv_weight, conv_bias, act_grad):
    count_tok = conv_in.shape[0]
    blocks = N_TP
    width = INNER_DEV
    saved = conv_in.reshape(count_tok, blocks, width).transpose(1, 0, 2)
    cotangent = act_grad.reshape(count_tok, blocks, width).transpose(1, 0, 2)
    taps = conv_weight.reshape(TAPS, blocks, width).transpose(1, 0, 2)
    offset = conv_bias.reshape(blocks, width)
    weight = proj_weight.reshape(D, blocks, width).transpose(1, 0, 2)
    start_sum = jnp.zeros((count_tok, D), jnp.float32)
    normalized_gradient, parts = lax.scan(channel_block, start_sum, (saved, cotangent, taps, offset, weight))
    taps_grad = parts[0].transpose(1, 0, 2).reshape(TAPS, blocks * width)
    bias_grad = parts[1].reshape(blocks * width)
    hidden_state = hidden_in.astype(jnp.float32)
    root_mean_square = jnp.sqrt(lax.optimization_barrier(jnp.mean(hidden_state * hidden_state, -1, keepdims=True)) + 1e-05)
    normalized_input = hidden_state / root_mean_square
    norm_gain_gradient = lax.optimization_barrier(jnp.sum(normalized_gradient * normalized_input, 0))
    scaled_gradient = norm_gain[None, :] * normalized_gradient
    mean_correction = lax.optimization_barrier(jnp.mean(scaled_gradient * normalized_input, -1, keepdims=True))
    hidden_input_gradient = ((scaled_gradient - normalized_input * mean_correction) / root_mean_square).astype(jnp.bfloat16)
    return (hidden_input_gradient, norm_gain_gradient, taps_grad, bias_grad)
```

```python
import jax
import jax.numpy as jnp
from jax import lax
from jax.sharding import PartitionSpec as P


def from_behind(block, axis, distance):
    devices = range(lax.axis_size(axis))
    route = [(i - distance, i) for i in devices if i - distance in devices]
    return lax.ppermute(block, axis, route)


def preact_of(padded, taps, offset, count_tok):
    tap_count = taps.shape[0]
    return offset[None, :] + sum(
        (
            taps[index][None, :] * padded[tap_count - 1 - index : tap_count - 1 - index + count_tok]
            for index in range(tap_count)
        )
    )


def grad_of(preact, cotangent):
    sigmoid_v = jax.nn.sigmoid(preact)
    return cotangent.astype(jnp.float32) * sigmoid_v * (1.0 + preact * (1.0 - sigmoid_v))


def xor_sum(value, axis):
    size = lax.axis_size(axis)
    if size & (size - 1):
        return lax.psum(value, axis)
    step = 1
    while step < size:
        value = value + lax.ppermute(value, axis, [(i, i ^ step) for i in range(size)])
        step *= 2
    return value


def line_scatter_parts(part, axis):
    size = lax.axis_size(axis)
    place = lax.axis_index(axis)
    rows = part.shape[0] // size

    def block(index):
        return lax.dynamic_slice_in_dim(part, jnp.clip(index, 0, size - 1) * rows, rows, 0)

    def joined(own, arrived):
        if arrived is None:
            return own
        return (own.astype(jnp.float32) + arrived.astype(jnp.float32)).astype(part.dtype)

    right = left = None
    for hop in range(1, size):
        send_right = joined(block(size - hop + place), right)
        send_left = joined(block(hop - size + place), left)
        right = lax.ppermute(send_right, axis, [(i, i + 1) for i in range(hop)])
        left = lax.ppermute(send_left, axis, [(size - 1 - i, size - 2 - i) for i in range(hop)])
        if hop < size - 1:
            yield None
    total = block(place).astype(jnp.float32)
    if right is not None:
        total = total + right.astype(jnp.float32) + left.astype(jnp.float32)
    yield total


CHUNKS = 2


def on_device(hidden_in, norm_gain, proj_weight, conv_in, conv_weight, conv_bias, act_grad):
    count_tok = conv_in.shape[0]
    tap_count = conv_weight.shape[0]
    edge_rows = tap_count - 1
    earlier = from_behind(conv_in[count_tok - edge_rows :], "ctx", 1)
    later = from_behind(jnp.concatenate([conv_in[:edge_rows], act_grad[:edge_rows]], 0), "ctx", -1)
    later_in, later_grad = later[:edge_rows], later[edge_rows:]
    padded = jnp.concatenate([earlier, conv_in], 0).astype(jnp.float32)
    preact = preact_of(padded, conv_weight, conv_bias, count_tok)
    pre_grad = grad_of(preact, act_grad)
    tail_pad = jnp.concatenate([conv_in[count_tok - edge_rows :], later_in], 0).astype(jnp.float32)
    tail_pre = preact_of(tail_pad, conv_weight, conv_bias, edge_rows)
    next_grad = grad_of(tail_pre, later_grad)
    after = jnp.concatenate([pre_grad, next_grad], 0)
    in_grad = sum(
        (
            conv_weight[index][None, :] * after[index : index + count_tok]
            for index in range(tap_count)
        )
    ).astype(jnp.bfloat16)
    in_grad = lax.optimization_barrier(in_grad)
    width = proj_weight.shape[0]
    chunk = width // CHUNKS
    streams = []
    for index in range(CHUNKS):
        part = lax.dot_general(
            in_grad,
            proj_weight[index * chunk : (index + 1) * chunk],
            (((1,), (1,)), ((), ())),
            preferred_element_type=jnp.float32,
        ).astype(jnp.bfloat16)
        streams.append(line_scatter_parts(lax.optimization_barrier(part), "tp"))
    sums = [None] * CHUNKS
    for _ in range(max(lax.axis_size("tp") - 1, 1)):
        for index in range(CHUNKS):
            sums[index] = next(streams[index])
    taps_part = jnp.stack(
        [
            jnp.sum(pre_grad * padded[edge_rows - index : edge_rows - index + count_tok], 0)
            for index in range(tap_count)
        ]
        + [jnp.sum(pre_grad, 0)],
        0,
    )
    taps_all = xor_sum(taps_part, "ctx")
    taps_grad, bias_grad = taps_all[:tap_count], taps_all[tap_count]
    normalized_gradient = jnp.concatenate(sums, 1)
    hidden_state = hidden_in.astype(jnp.float32)
    root_mean_square = jnp.sqrt(jnp.mean(hidden_state * hidden_state, -1, keepdims=True) + 1e-05)
    normalized_input = hidden_state / root_mean_square
    norm_gain_gradient = xor_sum(
        xor_sum(jnp.sum(normalized_gradient * normalized_input, 0), "ctx"), "tp"
    )
    scaled_gradient = norm_gain[None, :] * normalized_gradient
    mean_correction = jnp.mean(scaled_gradient * normalized_input, -1, keepdims=True)
    hidden_input_gradient = (
        (scaled_gradient - normalized_input * mean_correction) / root_mean_square
    ).astype(jnp.bfloat16)
    return (hidden_input_gradient, norm_gain_gradient, taps_grad, bias_grad)


def solution(mesh):
    return jax.shard_map(
        on_device,
        mesh=mesh,
        in_specs=(
            P(("ctx", "tp"), None),
            P(),
            P(None, "tp"),
            P("ctx", "tp"),
            P(None, "tp"),
            P("tp"),
            P("ctx", "tp"),
        ),
        out_specs=(P(("ctx", "tp"), None), P(), P(None, "tp"), P("tp")),
        check_vma=False,
    )
```

```python
import jax
import jax.numpy as jnp
from jax import lax
from jax.sharding import PartitionSpec as P


def from_behind(block, axis, distance):
    devices = range(lax.axis_size(axis))
    route = [(i - distance, i) for i in devices if i - distance in devices]
    return lax.ppermute(block, axis, route)


def preact_of(padded, taps, offset, count_tok):
    tap_count = taps.shape[0]
    return offset[None, :] + sum(
        (
            taps[index][None, :] * padded[tap_count - 1 - index : tap_count - 1 - index + count_tok]
            for index in range(tap_count)
        )
    )


def grad_of(preact, cotangent):
    sigmoid_v = jax.nn.sigmoid(preact)
    return cotangent.astype(jnp.float32) * sigmoid_v * (1.0 + preact * (1.0 - sigmoid_v))


def xor_sum(value, axis):
    size = lax.axis_size(axis)
    if size & (size - 1):
        return lax.psum(value, axis)
    step = 1
    while step < size:
        arrived = lax.ppermute(value, axis, [(i, i ^ step) for i in range(size)])
        value = value + arrived
        step *= 2
    return value


def line_scatter(parts, axis):
    size = lax.axis_size(axis)
    place = lax.axis_index(axis)
    rows = parts[0].shape[0] // size

    def block(part, index):
        return lax.dynamic_slice_in_dim(part, index * rows, rows, 0)

    sums = [block(part, place).astype(jnp.float32) for part in parts]
    last = [jnp.zeros(total.shape, part.dtype) for total, part in zip(sums, parts)]
    sent = list(last)
    first = None
    for target in range(size - 1, 0, -1):
        for index, part in enumerate(parts):
            moving = None
            for hop in range(target):
                own = block(part, jnp.where(place == hop, target, size - 1 - target))
                if moving is None:
                    moving = lax.optimization_barrier(own)
                else:
                    moving = (own.astype(jnp.float32) + moving.astype(jnp.float32)).astype(part.dtype)
                if target == 1:
                    sent[index] = moving
                moving = lax.ppermute(
                    moving, axis, [(hop, hop + 1), (size - 1 - hop, size - 2 - hop)]
                )
                if first is None:
                    first = moving
            if target > 1:
                sums[index] = sums[index] + moving.astype(jnp.float32)
            else:
                last[index] = moving
    return sums, last, sent, first


CHUNKS = 2


def on_device(hidden_in, norm_gain, proj_weight, conv_in, conv_weight, conv_bias, act_grad):
    count_tok = conv_in.shape[0]
    tap_count = conv_weight.shape[0]
    edge_rows = tap_count - 1
    size = lax.axis_size("tp")
    earlier = from_behind(conv_in[count_tok - edge_rows :], "ctx", 1)
    later = from_behind(jnp.concatenate([conv_in[:edge_rows], act_grad[:edge_rows]], 0), "ctx", -1)
    later_in, later_grad = later[:edge_rows], later[edge_rows:]
    padded = jnp.concatenate([earlier, conv_in], 0).astype(jnp.float32)
    preact = preact_of(padded, conv_weight, conv_bias, count_tok)
    pre_grad = grad_of(preact, act_grad)
    tail_pad = jnp.concatenate([conv_in[count_tok - edge_rows :], later_in], 0).astype(jnp.float32)
    tail_pre = preact_of(tail_pad, conv_weight, conv_bias, edge_rows)
    next_grad = grad_of(tail_pre, later_grad)
    after = jnp.concatenate([pre_grad, next_grad], 0)
    in_grad = sum(
        (
            conv_weight[index][None, :] * after[index : index + count_tok]
            for index in range(tap_count)
        )
    ).astype(jnp.bfloat16)
    in_grad, pre_grad, padded = lax.optimization_barrier((in_grad, pre_grad, padded))
    width = proj_weight.shape[0]
    chunk = width // CHUNKS
    parts = []
    for index in range(CHUNKS):
        part = lax.dot_general(
            in_grad,
            proj_weight[index * chunk : (index + 1) * chunk],
            (((1,), (1,)), ((), ())),
            preferred_element_type=jnp.float32,
        ).astype(jnp.bfloat16)
        parts.append(lax.optimization_barrier(part))
    sums, last, sent, first = line_scatter(parts, "tp")
    beside = lax.ppermute(hidden_in, "tp", [(1, 0), (size - 2, size - 1)])
    pre_grad, padded, hidden_in, _ = lax.optimization_barrier((pre_grad, padded, hidden_in, first))
    taps_part = jnp.stack(
        [
            jnp.sum(pre_grad * padded[edge_rows - index : edge_rows - index + count_tok], 0)
            for index in range(tap_count)
        ]
        + [jnp.sum(pre_grad, 0)],
        0,
    )
    taps_all = xor_sum(taps_part, "ctx")
    taps_grad, bias_grad = taps_all[:tap_count], taps_all[tap_count]

    def rms_of(hidden):
        return jnp.sqrt(jnp.mean(hidden * hidden, -1, keepdims=True) + 1e-05)

    hidden_state = hidden_in.astype(jnp.float32)
    root_mean_square = rms_of(hidden_state)
    normalized_input = hidden_state / root_mean_square
    beside = beside.astype(jnp.float32)
    normalized_beside = beside / rms_of(beside)
    gain_part = jnp.concatenate(
        [
            jnp.sum(
                sums[index] * normalized_input[:, index * chunk : (index + 1) * chunk]
                + sent[index].astype(jnp.float32)
                * normalized_beside[:, index * chunk : (index + 1) * chunk],
                0,
            )
            for index in range(CHUNKS)
        ]
    )
    norm_gain_gradient = xor_sum(xor_sum(gain_part, "ctx"), "tp")
    normalized_gradient = jnp.concatenate(
        [total + arrived.astype(jnp.float32) for total, arrived in zip(sums, last)], 1
    )
    scaled_gradient = norm_gain[None, :] * normalized_gradient
    mean_correction = jnp.mean(scaled_gradient * normalized_input, -1, keepdims=True)
    hidden_input_gradient = (
        (scaled_gradient - normalized_input * mean_correction) / root_mean_square
    ).astype(jnp.bfloat16)
    return (hidden_input_gradient, norm_gain_gradient, taps_grad, bias_grad)


def solution(mesh):
    return jax.shard_map(
        on_device,
        mesh=mesh,
        in_specs=(
            P(("ctx", "tp"), None),
            P(),
            P(None, "tp"),
            P("ctx", "tp"),
            P(None, "tp"),
            P("tp"),
            P("ctx", "tp"),
        ),
        out_specs=(P(("ctx", "tp"), None), P(), P(None, "tp"), P("tp")),
        check_vma=False,
    )
```

```python
import jax
import jax.numpy as jnp
from jax import lax
from jax.sharding import PartitionSpec as P


def from_behind(block, axis, distance):
    devices = range(lax.axis_size(axis))
    route = [(i - distance, i) for i in devices if i - distance in devices]
    return lax.ppermute(block, axis, route)


def preact_of(padded, taps, offset, count_tok):
    tap_count = taps.shape[0]
    return offset[None, :] + sum(
        (
            taps[index][None, :] * padded[tap_count - 1 - index : tap_count - 1 - index + count_tok]
            for index in range(tap_count)
        )
    )


def grad_of(preact, cotangent):
    sigmoid_v = jax.nn.sigmoid(preact)
    return cotangent.astype(jnp.float32) * sigmoid_v * (1.0 + preact * (1.0 - sigmoid_v))


def xor_sum(value, axis):
    size = lax.axis_size(axis)
    if size & (size - 1):
        return lax.psum(value, axis)
    step = 1
    while step < size:
        arrived = lax.ppermute(value, axis, [(i, i ^ step) for i in range(size)])
        value = value + arrived
        step *= 2
    return value


def line_scatter(parts, axis):
    size = lax.axis_size(axis)
    rows = parts[0].shape[0] // size
    places = [lax.optimization_barrier((lax.axis_index(axis), part))[0] for part in parts]

    def block(part, index):
        return lax.dynamic_slice_in_dim(part, index * rows, rows, 0)

    sums = [block(part, place).astype(jnp.float32) for part, place in zip(parts, places)]
    last = [jnp.zeros(total.shape, part.dtype) for total, part in zip(sums, parts)]
    sent = list(last)
    first = None
    for target in range(size - 1, 0, -1):
        for index, part in enumerate(parts):
            moving = None
            for hop in range(target):
                own = block(part, jnp.where(places[index] == hop, target, size - 1 - target))
                if moving is None:
                    moving = lax.optimization_barrier(own)
                else:
                    moving = (own.astype(jnp.float32) + moving.astype(jnp.float32)).astype(part.dtype)
                if target == 1:
                    sent[index] = moving
                moving = lax.ppermute(
                    moving, axis, [(hop, hop + 1), (size - 1 - hop, size - 2 - hop)]
                )
                if first is None:
                    first = moving
            if target > 1:
                sums[index] = sums[index] + moving.astype(jnp.float32)
            else:
                last[index] = moving
    return sums, last, sent, first


CHUNKS = 2


def on_device(hidden_in, norm_gain, proj_weight, conv_in, conv_weight, conv_bias, act_grad):
    count_tok = conv_in.shape[0]
    tap_count = conv_weight.shape[0]
    edge_rows = tap_count - 1
    size = lax.axis_size("tp")
    earlier = from_behind(conv_in[count_tok - edge_rows :], "ctx", 1)
    later = from_behind(jnp.concatenate([conv_in[:edge_rows], act_grad[:edge_rows]], 0), "ctx", -1)
    beside = lax.ppermute(hidden_in, "tp", [(1, 0), (size - 2, size - 1)])
    later_in, later_grad = later[:edge_rows], later[edge_rows:]
    padded = jnp.concatenate([earlier, conv_in], 0).astype(jnp.float32)
    preact = preact_of(padded, conv_weight, conv_bias, count_tok)
    pre_grad = grad_of(preact, act_grad)
    tail_pad = jnp.concatenate([conv_in[count_tok - edge_rows :], later_in], 0).astype(jnp.float32)
    tail_pre = preact_of(tail_pad, conv_weight, conv_bias, edge_rows)
    next_grad = grad_of(tail_pre, later_grad)
    after = jnp.concatenate([pre_grad, next_grad], 0)
    in_grad = sum(
        (
            conv_weight[index][None, :] * after[index : index + count_tok]
            for index in range(tap_count)
        )
    ).astype(jnp.bfloat16)
    in_grad, pre_grad, padded = lax.optimization_barrier((in_grad, pre_grad, padded))
    width = proj_weight.shape[0]
    chunk = width // CHUNKS
    parts = []
    for index in range(CHUNKS):
        part = lax.dot_general(
            in_grad,
            proj_weight[index * chunk : (index + 1) * chunk],
            (((1,), (1,)), ((), ())),
            preferred_element_type=jnp.float32,
        ).astype(jnp.bfloat16)
        parts.append(lax.optimization_barrier(part))
    sums, last, sent, first = line_scatter(parts, "tp")
    pre_grad, padded, hidden_in, beside, _ = lax.optimization_barrier(
        (pre_grad, padded, hidden_in, beside, first)
    )
    taps_part = jnp.stack(
        [
            jnp.sum(pre_grad * padded[edge_rows - index : edge_rows - index + count_tok], 0)
            for index in range(tap_count)
        ]
        + [jnp.sum(pre_grad, 0)],
        0,
    )
    taps_all = xor_sum(taps_part, "ctx")
    taps_grad, bias_grad = taps_all[:tap_count], taps_all[tap_count]

    def rms_of(hidden):
        return jnp.sqrt(jnp.mean(hidden * hidden, -1, keepdims=True) + 1e-05)

    hidden_state = hidden_in.astype(jnp.float32)
    root_mean_square = rms_of(hidden_state)
    normalized_input = hidden_state / root_mean_square
    beside = beside.astype(jnp.float32)
    normalized_beside = beside / rms_of(beside)
    sums = lax.optimization_barrier(sums)
    gain_part = [
        jnp.sum(
            sums[index] * normalized_input[:, index * chunk : (index + 1) * chunk]
            + sent[index].astype(jnp.float32)
            * normalized_beside[:, index * chunk : (index + 1) * chunk],
            0,
        )
        for index in range(CHUNKS)
    ]
    gain_part = lax.optimization_barrier(jnp.concatenate(gain_part))
    gain_part, last = lax.optimization_barrier((xor_sum(gain_part, "ctx"), last))
    norm_gain_gradient = xor_sum(gain_part, "tp")
    normalized_gradient = jnp.concatenate(
        [total + arrived.astype(jnp.float32) for total, arrived in zip(sums, last)], 1
    )
    scaled_gradient = norm_gain[None, :] * normalized_gradient
    mean_correction = jnp.mean(scaled_gradient * normalized_input, -1, keepdims=True)
    hidden_input_gradient = (
        (scaled_gradient - normalized_input * mean_correction) / root_mean_square
    ).astype(jnp.bfloat16)
    return (hidden_input_gradient, norm_gain_gradient, taps_grad, bias_grad)


def solution(mesh):
    return jax.shard_map(
        on_device,
        mesh=mesh,
        in_specs=(
            P(("ctx", "tp"), None),
            P(),
            P(None, "tp"),
            P("ctx", "tp"),
            P(None, "tp"),
            P("tp"),
            P("ctx", "tp"),
        ),
        out_specs=(P(("ctx", "tp"), None), P(), P(None, "tp"), P("tp")),
        check_vma=False,
    )
```

```python
import jax
import jax.numpy as jnp
from jax import lax
from jax.sharding import PartitionSpec as P


def from_behind(block, axis, distance):
    devices = range(lax.axis_size(axis))
    route = [(i - distance, i) for i in devices if i - distance in devices]
    return lax.ppermute(block, axis, route)


def preact_of(padded, taps, offset, count_tok):
    tap_count = taps.shape[0]
    return offset[None, :] + sum(
        (
            taps[index][None, :] * padded[tap_count - 1 - index : tap_count - 1 - index + count_tok]
            for index in range(tap_count)
        )
    )


def grad_of(preact, cotangent):
    sigmoid_v = jax.nn.sigmoid(preact)
    return cotangent.astype(jnp.float32) * sigmoid_v * (1.0 + preact * (1.0 - sigmoid_v))


def xor_sum(value, axis):
    size = lax.axis_size(axis)
    if size & (size - 1):
        return lax.psum(value, axis)
    step = 1
    while step < size:
        arrived = lax.ppermute(value, axis, [(i, i ^ step) for i in range(size)])
        value = value + arrived
        step *= 2
    return value


def line_scatter_parts(part, axis):
    size = lax.axis_size(axis)
    place = lax.axis_index(axis)
    rows = part.shape[0] // size

    def block(index):
        return lax.dynamic_slice_in_dim(part, jnp.clip(index, 0, size - 1) * rows, rows, 0)

    def joined(own, arrived):
        if arrived is None:
            return own
        return (own.astype(jnp.float32) + arrived.astype(jnp.float32)).astype(part.dtype)

    right = left = None
    for hop in range(1, size):
        send_right = joined(block(size - hop + place), right)
        send_left = joined(block(hop - size + place), left)
        send_right, send_left = lax.optimization_barrier((send_right, send_left))
        right = lax.ppermute(send_right, axis, [(i, i + 1) for i in range(hop)])
        left = lax.ppermute(send_left, axis, [(size - 1 - i, size - 2 - i) for i in range(hop)])
        if hop < size - 1:
            yield right
    total = block(place).astype(jnp.float32)
    if right is not None:
        total = total + right.astype(jnp.float32) + left.astype(jnp.float32)
    yield total


CHUNKS = 2


def on_device(hidden_in, norm_gain, proj_weight, conv_in, conv_weight, conv_bias, act_grad):
    count_tok = conv_in.shape[0]
    tap_count = conv_weight.shape[0]
    edge_rows = tap_count - 1
    earlier = from_behind(conv_in[count_tok - edge_rows :], "ctx", 1)
    later = from_behind(jnp.concatenate([conv_in[:edge_rows], act_grad[:edge_rows]], 0), "ctx", -1)
    later_in, later_grad = later[:edge_rows], later[edge_rows:]
    padded = jnp.concatenate([earlier, conv_in], 0).astype(jnp.float32)
    preact = preact_of(padded, conv_weight, conv_bias, count_tok)
    pre_grad = grad_of(preact, act_grad)
    tail_pad = jnp.concatenate([conv_in[count_tok - edge_rows :], later_in], 0).astype(jnp.float32)
    tail_pre = preact_of(tail_pad, conv_weight, conv_bias, edge_rows)
    next_grad = grad_of(tail_pre, later_grad)
    after = jnp.concatenate([pre_grad, next_grad], 0)
    in_grad = sum(
        (
            conv_weight[index][None, :] * after[index : index + count_tok]
            for index in range(tap_count)
        )
    ).astype(jnp.bfloat16)
    in_grad, pre_grad, padded = lax.optimization_barrier((in_grad, pre_grad, padded))
    width = proj_weight.shape[0]
    chunk = width // CHUNKS
    streams = []
    for index in range(CHUNKS):
        part = lax.dot_general(
            in_grad,
            proj_weight[index * chunk : (index + 1) * chunk],
            (((1,), (1,)), ((), ())),
            preferred_element_type=jnp.float32,
        ).astype(jnp.bfloat16)
        streams.append(line_scatter_parts(lax.optimization_barrier(part), "tp"))
    sums = [None] * CHUNKS
    first = None
    for _ in range(max(lax.axis_size("tp") - 1, 1)):
        for index in range(CHUNKS):
            sums[index] = next(streams[index])
            first = sums[index] if first is None else first
    pre_grad, padded, hidden_in, _ = lax.optimization_barrier((pre_grad, padded, hidden_in, first))
    taps_part = jnp.stack(
        [
            jnp.sum(pre_grad * padded[edge_rows - index : edge_rows - index + count_tok], 0)
            for index in range(tap_count)
        ]
        + [jnp.sum(pre_grad, 0)],
        0,
    )
    taps_all = xor_sum(taps_part, "ctx")
    taps_grad, bias_grad = taps_all[:tap_count], taps_all[tap_count]
    normalized_gradient = jnp.concatenate(sums, 1)
    hidden_state = hidden_in.astype(jnp.float32)
    root_mean_square = jnp.sqrt(jnp.mean(hidden_state * hidden_state, -1, keepdims=True) + 1e-05)
    normalized_input = hidden_state / root_mean_square
    norm_gain_gradient = xor_sum(
        xor_sum(jnp.sum(normalized_gradient * normalized_input, 0), "ctx"), "tp"
    )
    scaled_gradient = norm_gain[None, :] * normalized_gradient
    mean_correction = jnp.mean(scaled_gradient * normalized_input, -1, keepdims=True)
    hidden_input_gradient = (
        (scaled_gradient - normalized_input * mean_correction) / root_mean_square
    ).astype(jnp.bfloat16)
    return (hidden_input_gradient, norm_gain_gradient, taps_grad, bias_grad)


def solution(mesh):
    return jax.shard_map(
        on_device,
        mesh=mesh,
        in_specs=(
            P(("ctx", "tp"), None),
            P(),
            P(None, "tp"),
            P("ctx", "tp"),
            P(None, "tp"),
            P("tp"),
            P("ctx", "tp"),
        ),
        out_specs=(P(("ctx", "tp"), None), P(), P(None, "tp"), P("tp")),
        check_vma=False,
    )
```
